32 devices in a mesh: grp: 2 (over y), seq: 4 (over z), head: 4 (over x, core).
Axes of the slice: x: 2, y: 2, z: 4, core: 2. Of those that a mesh axis runs over, the one named last changes fastest.
Arguments:
- token_queries: bfloat16 [4, 1024, 4096], P('grp', 'seq', 'head'), parts along dimension 0, may hold values from -6 to 6
- token_keys: bfloat16 [4, 1024, 4096], P('grp', 'seq', 'head'), parts along dimension 0, may hold values from -6 to 6
- token_values: bfloat16 [4, 1024, 4096], P('grp', 'seq', 'head'), parts along dimension 0, may hold values from -6 to 6
- step_size: float32 [8, 4, 1024], P('head', 'grp', 'seq'), parts along dimension 1, may hold values from 0.5 to 9
- fast_weights: float32 [6, 8, 512, 512], P('grp', 'head', 'seq'), parts along dimension 0, may hold values from -0.25 to 0.25
- momentum: float32 [6, 8, 512, 512], P('grp', 'head', 'seq'), parts along dimension 0, may hold values from -0.1875 to 0.1875
- fast_gain: float32 [8, 512], P('head'), may hold values from 0.5 to 1.5
Outputs:
- layer_out: bfloat16 [4, 1024, 4096], P('grp', 'seq', 'head'), parts along dimension 0
- new_weights: float32 [6, 8, 512, 512], P('grp', 'head', 'seq'), parts along dimension 0
- new_momentum: float32 [6, 8, 512, 512], P('grp', 'head', 'seq'), parts along dimension 0
The draws below stay inside these ranges and needn't reach their ends.
There are 2 independent parts, one for each index of `grp`. The reference program is written for one: setup_inputs(seed, part) draws one part's arguments, and reference() takes and returns one part's arrays. A program takes and returns all parts, laid end to end along the dimension named above; an argument that names none is the same for every part. Nothing has to cross between parts.
All inputs are finite; a program needn't handle non-finite values.
Results may differ from the reference program's by a relative error of at most 0.025.
Values may be sent and summed in bfloat16 or wider, within the bound.
No kernel may reach another device: no remote copies, remote signals or barrier semaphores. Data moves between devices by JAX's collectives and lax.ppermute only.
A program may use at most 64 MiB of HBM per device.

```python
import math
import jax
import jax.numpy as jnp
from jax import lax

HD = 128
FH = 8
FD = 512
WINDOW = 256
CH_DEV = 256
GROUP = 1024
FEAT = 4096
N_SEQ = 4


def token_field(key, salt):
    noise_key, scale_key = jax.random.split(jax.random.fold_in(key, salt))
    noise = jax.random.normal(noise_key, (2 * GROUP, FH * FD), jnp.float32)
    scales = jnp.exp(jax.random.uniform(scale_key, (2 * GROUP, 1), jnp.float32, jnp.log(0.5), jnp.log(2.0)))
    return jnp.clip(noise * scales, -6.0, 6.0)


def draw_token_queries(key, part):
    field = token_field(key, 11)
    return field.reshape(2, GROUP, FH * FD).astype(jnp.bfloat16)


def draw_token_keys(key, part):
    field = token_field(key, 13)
    return field.reshape(2, GROUP, FH * FD).astype(jnp.bfloat16)


def draw_step_size(key, part):
    position = jnp.arange(GROUP, dtype=jnp.float32) / GROUP
    ramp = 1.0 + 2.0 * position
    jitter = jnp.exp(jax.random.uniform(jax.random.fold_in(key, 17), (FH, 2, GROUP), jnp.float32, jnp.log(0.5), 0.0))
    return (ramp[None, None, :] * jitter).astype(jnp.float32)


def raised(values, rng, source, target, parts, factor):
    def block_of(dim):
        return (jnp.arange(values.shape[dim]) // (values.shape[dim] // parts)).reshape((-1,) + (1,) * (values.ndim - 1 - dim))

    first = jax.random.permutation(rng, parts)[block_of(target)]
    other_side = (block_of(target) + parts // 2) % parts
    return jnp.where((block_of(source) == first) | (block_of(source) == other_side), factor * values, values)


def steps_of(rng, dims, cuts, smallest, largest):
    factor_of, own = 1.0, jax.random.fold_in(rng, 6)
    for dim, shards_of in cuts:
        steps = jnp.exp(jax.random.uniform(jax.random.fold_in(own, dim), (shards_of,), jnp.float32, smallest / len(cuts), largest / len(cuts)))
        factor_of = factor_of * jnp.repeat(steps, dims[dim] // shards_of).reshape([-1 if axis == dim else 1 for axis in range(len(dims))])
    return factor_of


def gaussian(own_key, dims, width, most, shards=(), held_as=jnp.bfloat16):
    drawn = jax.random.normal(own_key, dims, jnp.float32) * width
    if len(shards) > 0:
        drawn = steps_of(own_key, dims, shards, -0.22, 0.18) * drawn
    return jnp.clip(drawn, min=-most, max=most).astype(held_as)


def bell_draw_with(own_key, extent, width, limit, pieces, heavy, held_as=jnp.bfloat16):
    values = width * jax.random.normal(own_key, extent, jnp.float32)
    if pieces:
        values = values * steps_of(own_key, extent, pieces, -0.22, 0.18)
    return jnp.clip(raised(values, jax.random.fold_in(own_key, 3), *heavy), -limit, limit).astype(held_as)


def setup_inputs(seed: int = 0, part: int = 0) -> dict:
    arg_keys = jax.random.split(jax.random.key(seed), 8)
    part_splits = jax.random.split(jax.random.fold_in(arg_keys[7], part), 8)
    token_queries = draw_token_queries(jax.random.fold_in(jax.random.fold_in(arg_keys[7], part), 71), part)
    token_keys = draw_token_keys(jax.random.fold_in(jax.random.fold_in(arg_keys[7], part), 71), part)
    token_values = bell_draw_with(part_splits[2], (2, GROUP, FEAT), 1.0, 6.0, ((1, 4), (2, 4)), (1, 2, 4, 2.0))
    step_size = draw_step_size(jax.random.fold_in(jax.random.fold_in(arg_keys[7], part), 71), part)
    fast_weights = gaussian(part_splits[4], (3, FH, FD, FD), FD ** -0.5, 0.25, ((1, 4), (2, 4)), jnp.float32)
    momentum = gaussian(part_splits[5], (3, FH, FD, FD), (0.6 / GROUP ** 0.5), 0.1875, ((1, 4), (2, 4)), jnp.float32)
    fast_gain = jnp.clip(1.0 + 0.1 * jax.random.normal(arg_keys[6], (FH, FD), jnp.float32), 0.5, 1.5)
    return dict(token_queries=token_queries, token_keys=token_keys, token_values=token_values, step_size=step_size, fast_weights=fast_weights, momentum=momentum, fast_gain=fast_gain)


EPSILON = 1e-06
MOMENT_DECAY = 0.9
STEP_RATE = 0.02

def rms_rows(values):
    return values * lax.rsqrt(lax.optimization_barrier(jnp.mean(values * values, axis=-1, keepdims=True)) + EPSILON)

def attention(token_queries, token_keys, token_values):
    blocks = 2 * GROUP // CH_DEV
    head_count = FH * FD // HD
    query_blocks = token_queries.reshape(blocks, CH_DEV, head_count, HD)
    key_blocks = token_keys.reshape(blocks, CH_DEV, head_count, HD)
    value_blocks = token_values.reshape(blocks, CH_DEV, head_count, HD)
    key_prior = jnp.concatenate([jnp.zeros_like(key_blocks[:1]), key_blocks[:-1]], axis=0)[:, CH_DEV - WINDOW:]
    value_prior = jnp.concatenate([jnp.zeros_like(value_blocks[:1]), value_blocks[:-1]], axis=0)[:, CH_DEV - WINDOW:]
    query_pos = jnp.arange(CH_DEV, dtype=jnp.int32)[:, None]
    key_pos = jnp.arange(WINDOW + CH_DEV, dtype=jnp.int32)[None, :] - WINDOW
    band = (key_pos <= query_pos) & (key_pos > query_pos - WINDOW)
    score_scale = 1.0 / math.sqrt(HD)

    def one_block(inputs):
        query_block, key_block, value_block, key_back, value_back, index = inputs
        key_all = jnp.concatenate([key_back, key_block], 0).astype(jnp.float32)
        value_all = jnp.concatenate([value_back, value_block], 0).astype(jnp.float32)
        scores = jnp.einsum('qhd,khd->hqk', query_block.astype(jnp.float32), key_all) * score_scale
        allowed = band & ((key_pos >= 0) | (index > 0))
        scores = jnp.where(allowed[None], scores, -1e+30)
        top = lax.optimization_barrier(jnp.max(scores, axis=-1, keepdims=True))
        expo = jnp.exp(scores - top)
        probs = (expo / lax.optimization_barrier(jnp.sum(expo, axis=-1, keepdims=True))).astype(jnp.bfloat16)
        mixed = jnp.einsum('hqk,khd->qhd', probs.astype(jnp.float32), value_all)
        return mixed.reshape(CH_DEV, head_count * HD)
    result = lax.map(one_block, (query_blocks, key_blocks, value_blocks, key_prior, value_prior, jnp.arange(blocks, dtype=jnp.int32)))
    return result.reshape(2, GROUP, head_count * HD)

def shard_rows(values):
    return values.astype(jnp.float32).reshape(N_SEQ, CH_DEV, FD)

def fast_head(inputs):
    query_head, key_head, value_head, rates, weights, moment, gain = inputs
    results = []
    for period in range(2):
        casted = weights.astype(jnp.bfloat16)
        key_norm = rms_rows(key_head[period].astype(jnp.float32)).astype(jnp.bfloat16)
        gate_pre = jnp.dot(key_norm, casted[0].T, preferred_element_type=jnp.float32)
        up_pre = jnp.dot(key_norm, casted[1].T, preferred_element_type=jnp.float32)
        sigma = jax.nn.sigmoid(gate_pre)
        active = gate_pre * sigma
        slope = sigma * (1.0 + gate_pre * (1.0 - sigma))
        hidden = (active * up_pre).astype(jnp.bfloat16)
        targets = (rates[period][:, None] * value_head[period].astype(jnp.float32)).astype(jnp.bfloat16)
        back = -jnp.dot(targets, casted[2], preferred_element_type=jnp.float32)
        d_gate = (back * up_pre * slope).astype(jnp.bfloat16)
        d_up = (back * active).astype(jnp.bfloat16)
        g_gate = jnp.einsum('sti,stj->sij', shard_rows(d_gate), shard_rows(key_norm))
        g_up = jnp.einsum('sti,stj->sij', shard_rows(d_up), shard_rows(key_norm))
        g_down = -jnp.einsum('sto,sth->soh', shard_rows(targets), shard_rows(hidden))
        partial_value = jnp.stack([g_gate, g_up, g_down], axis=1)
        summed = lax.optimization_barrier(jnp.sum(lax.optimization_barrier(partial_value.astype(jnp.bfloat16)).astype(jnp.float32), axis=0))
        rate_total = jnp.sum(rates[period])
        moment = MOMENT_DECAY * moment + summed / rate_total
        weights = weights - STEP_RATE * rms_rows(moment)
        casted = weights.astype(jnp.bfloat16)
        query_norm = rms_rows(query_head[period].astype(jnp.float32)).astype(jnp.bfloat16)
        gate_q = jnp.dot(query_norm, casted[0].T, preferred_element_type=jnp.float32)
        up_q = jnp.dot(query_norm, casted[1].T, preferred_element_type=jnp.float32)
        hidden_q = (jax.nn.silu(gate_q) * up_q).astype(jnp.bfloat16)
        result = jnp.dot(hidden_q, casted[2].T, preferred_element_type=jnp.float32)
        results.append(rms_rows(result) * gain[None, :])
    return (jnp.stack(results), weights, moment)

def split_heads(values):
    return jnp.moveaxis(values.reshape(2, GROUP, FH, FD), 2, 0)

def reference(token_queries, token_keys, token_values, step_size, fast_weights, momentum, fast_gain):
    mixed = attention(token_queries, token_keys, token_values)
    fast_out, weights, moment = lax.map(fast_head, (split_heads(token_queries), split_heads(token_keys), split_heads(token_values), step_size, jnp.moveaxis(fast_weights, 1, 0), jnp.moveaxis(momentum, 1, 0), fast_gain))
    fast_out = jnp.moveaxis(fast_out, 0, 2).reshape(2, GROUP, FH * FD)
    layer_out = (mixed + fast_out).astype(jnp.bfloat16)
    return (layer_out, jnp.moveaxis(weights, 0, 1), jnp.moveaxis(moment, 0, 1))
```

```python
import functools
import math

import jax
import jax.numpy as jnp
from jax import lax
from jax.experimental import pallas as pl
from jax.experimental.pallas import tpu as pltpu
from jax.sharding import PartitionSpec as P

HD = 128
WINDOW = 256
CORES = 2


EPSILON = 1e-06
MOMENT_DECAY = 0.9
STEP_RATE = 0.02


def rms_rows(values):
    return values * lax.rsqrt(jnp.mean(values * values, axis=-1, keepdims=True) + EPSILON)


def routes(seq_size, head_size, turn):
    pairs = []
    for z in range(seq_size):
        for h in range(head_size):
            chip_axis, core = divmod(h, CORES)
            target = core * CORES + (turn + z) % CORES
            pairs.append((z * head_size + h, target * head_size + chip_axis * CORES + z // CORES))
    return pairs


def partners(seq_size, head_size):
    count = seq_size * head_size
    return [(i, i // CORES * CORES + (i + 1) % CORES) for i in range(count)]


def mm(left, right, dims):
    return lax.dot_general(left, right, (dims, ((), ())), preferred_element_type=jnp.float32)


NN = ((1,), (0,))
NT = ((1,), (1,))
TN = ((0,), (0,))


def place():
    parity = lax.rem(lax.axis_index("seq"), CORES)
    core = lax.rem(lax.axis_index("head"), CORES)
    return parity, core


def learn(kv_refs, rate_refs, period, casted, moment_of, weight_of, emit, scratch):
    key_s, target_s, gate_s, up_s, hidden_s = scratch
    rows = kv_refs[0].shape[1]
    width = kv_refs[0].shape[2]
    rate_total = jnp.zeros((1, 1), jnp.float32)
    for i, (kv, rate) in enumerate(zip(kv_refs, rate_refs)):
        at = pl.ds(i * rows, rows)
        rate_row = rate[period : period + 1, :]
        rate_total = rate_total + jnp.sum(rate_row, axis=1, keepdims=True)
        rate_col = jnp.broadcast_to(rate_row, (HD, rows)).T
        rate_all = jnp.concatenate([rate_col] * (width // HD), axis=1)
        key_norm = rms_rows(kv[0].astype(jnp.float32)).astype(jnp.bfloat16)
        target = (rate_all * kv[1].astype(jnp.float32)).astype(jnp.bfloat16)
        gate_pre = mm(key_norm, casted(0), NT)
        up_pre = mm(key_norm, casted(1), NT)
        back = -mm(target, casted(2), NN)
        sigma = jax.nn.sigmoid(gate_pre)
        active = gate_pre * sigma
        slope = sigma * (1.0 + gate_pre * (1.0 - sigma))
        key_s[at, :] = key_norm
        target_s[at, :] = target
        hidden_s[at, :] = (active * up_pre).astype(jnp.bfloat16)
        gate_s[at, :] = (back * up_pre * slope).astype(jnp.bfloat16)
        up_s[at, :] = (back * active).astype(jnp.bfloat16)
    scale = 1.0 / rate_total
    for i, (left, right, sign) in enumerate(
        ((gate_s, key_s, 1.0), (up_s, key_s, 1.0), (target_s, hidden_s, -1.0))
    ):
        summed = mm(left[...], right[...], TN)
        moment = MOMENT_DECAY * moment_of(i) + (sign * scale) * summed
        weights = weight_of(i) - STEP_RATE * rms_rows(moment)
        emit(i, weights, moment)


def first_kernel(*refs):
    kv_refs, rate_refs, wm_refs = (refs[0:4], refs[4:8], refs[8:12])
    weight_out, moment_out, casted_out = refs[12:15]
    full, scratch = refs[15], refs[16:]
    parity, core = place()
    rows = wm_refs[0].shape[1]
    for side in range(CORES):
        owner = core if side == 0 else 1 - core
        for half in range(CORES):
            even_first = jnp.broadcast_to(parity == half, wm_refs[0].shape[1:])
            for i in range(wm_refs[0].shape[0]):
                block = jnp.where(even_first, wm_refs[2 * side][i], wm_refs[2 * side + 1][i])
                full[i, pl.ds(pl.multiple_of((owner * CORES + half) * rows, rows), rows), :] = block

    def emit(i, weights, moment):
        weight_out[i] = weights
        moment_out[i] = moment
        casted_out[i] = weights.astype(jnp.bfloat16)

    learn(
        kv_refs,
        rate_refs,
        0,
        lambda i: full[i],
        lambda i: full[3 + i].astype(jnp.float32),
        lambda i: full[i].astype(jnp.float32),
        emit,
        scratch,
    )


def second_kernel(*refs):
    kv_refs, rate_refs = (refs[0:4], refs[4:8])
    weight_in, moment_in, casted_in = refs[8:11]
    casted_out, back_refs = refs[11], refs[12:14]
    whole, scratch = refs[14], refs[15:]
    parity, core = place()
    rows = back_refs[0].shape[1]

    def emit(i, weights, moment):
        casted_out[i] = weights.astype(jnp.bfloat16)
        whole[...] = moment.astype(jnp.bfloat16)
        for turn in range(CORES):
            half = lax.rem(parity + turn, CORES)
            at = pl.ds(pl.multiple_of((core * CORES + half) * rows, rows), rows)
            back_refs[turn][i] = casted_out[i, at, :]
            back_refs[turn][3 + i] = whole[at, :]

    learn(
        kv_refs,
        rate_refs,
        1,
        lambda i: casted_in[i],
        lambda i: moment_in[i],
        lambda i: weight_in[i],
        emit,
        scratch,
    )


def query_kernel(period, *refs):
    query_refs, kv_refs = (refs[0:2], refs[2:6])
    before_refs = refs[6:8]
    casted, gain_own, gain_other = refs[8:11]
    out_refs = refs[11:13]
    parity, core = place()
    z = lax.axis_index("seq")
    rows, width = query_refs[0].shape
    mine = lax.div(z, CORES) == core
    gain_rows = jnp.where(jnp.broadcast_to(mine, gain_own.shape), gain_own[...], gain_other[...])
    gain = jnp.where(jnp.broadcast_to(parity == 0, (1, width)), gain_rows[0:1], gain_rows[1:2])
    q_pos = lax.broadcasted_iota(jnp.int32, (rows, rows), 0)
    k_pos = lax.broadcasted_iota(jnp.int32, (rows, rows), 1)
    own_side = k_pos <= q_pos
    flip = jnp.broadcast_to(parity == 0, (rows, HD))
    late = jnp.broadcast_to(core == 1, (rows, HD))
    alive = jnp.logical_or(core == 1, period > 0)
    for turn in range(CORES):
        odd = lax.rem(parity + turn, CORES) == 1
        odd_rows = jnp.broadcast_to(odd, (rows, HD))
        live = jnp.broadcast_to(jnp.logical_or(odd, alive), (rows, rows))
        query_norm = rms_rows(query_refs[turn][...].astype(jnp.float32)).astype(jnp.bfloat16)
        gate_pre = mm(query_norm, casted[0], NT)
        up_pre = mm(query_norm, casted[1], NT)
        hidden = (gate_pre * jax.nn.sigmoid(gate_pre) * up_pre).astype(jnp.bfloat16)
        fast = rms_rows(mm(hidden, casted[2], NT)) * gain
        for head in range(width // HD):
            at = slice(head * HD, (head + 1) * HD)

            def prior(which):
                here = jnp.where(flip, kv_refs[3][which, :, at], kv_refs[2][which, :, at])
                there = jnp.where(flip, before_refs[1][which, :, at], before_refs[0][which, :, at])
                halo = jnp.where(late, here, there)
                return jnp.where(odd_rows, kv_refs[1 - turn][which, :, at], halo)

            query = query_refs[turn][:, at]
            own = mm(query, kv_refs[turn][0, :, at], NT)
            back = mm(query, prior(0), NT)
            back = jnp.where(live, back, -1e30 * math.sqrt(HD))
            scores = jnp.where(own_side, own, back) * (1.0 / math.sqrt(HD))
            top = jnp.max(scores, axis=-1, keepdims=True)
            expo = jnp.exp(scores - top)
            probs = expo * (1.0 / jnp.sum(expo, axis=-1, keepdims=True))
            probs_own = jnp.where(own_side, probs, 0.0).astype(jnp.bfloat16)
            probs_back = jnp.where(own_side, 0.0, probs).astype(jnp.bfloat16)
            mixed = mm(probs_own, kv_refs[turn][1, :, at], NN) + mm(probs_back, prior(1), NN)
            out_refs[turn][:, at] = (mixed + fast[:, at]).astype(jnp.bfloat16)


def in_vmem(count):
    return [pl.BlockSpec(memory_space=pltpu.VMEM)] * count


def call(kernel, operands, outs, scratch, name, flops):
    moved = sum(x.size * x.dtype.itemsize for x in (*operands, *outs))
    return pl.pallas_call(
        kernel,
        out_shape=tuple(outs),
        in_specs=in_vmem(len(operands)),
        out_specs=tuple(in_vmem(len(outs))),
        scratch_shapes=scratch,
        cost_estimate=pl.CostEstimate(flops=flops, transcendentals=0, bytes_accessed=moved),
        name=name,
    )(*operands)


def head_parallel(token_queries, token_keys, token_values, step_size, fast_weights, momentum, fast_gain):
    periods, rows, features = token_queries.shape
    width = fast_weights.shape[3]
    seq_size, head_size = (lax.axis_size("seq"), lax.axis_size("head"))
    axes = ("seq", "head")
    out_routes = [routes(seq_size, head_size, turn) for turn in range(CORES)]
    home_routes = [[(b, a) for a, b in route] for route in out_routes]
    swap_route = partners(seq_size, head_size)
    even = lax.rem(lax.axis_index("seq"), CORES) == 0

    def swap(value):
        return lax.ppermute(value, axes, swap_route)

    def by_turn(first, second):
        return (jnp.where(even, first, second), jnp.where(even, second, first))

    def send(pair):
        return [lax.ppermute(value, axes, route) for value, route in zip(pair, out_routes)]

    def send_home(pair):
        return [lax.ppermute(value, axes, route) for value, route in zip(pair, home_routes)]

    def both(pair):
        return [*pair, *[swap(value) for value in pair]]

    def key_values(period):
        stacked = jnp.stack([token_keys[period], token_values[period]])
        return by_turn(stacked[..., :width], stacked[..., width:])

    def queries(period):
        return by_turn(token_queries[period, :, :width], token_queries[period, :, width:])

    state = jnp.concatenate([fast_weights, momentum]).astype(jnp.bfloat16)
    gain_other = swap(fast_gain)
    rate_sent = send(by_turn(step_size[0], step_size[1]))
    kv_sent = [send(key_values(0))]
    state_sent = send(by_turn(state[:, 0], state[:, 1]))
    query_sent = [send(queries(0))]
    kv_sent.append(send(key_values(1)))
    query_sent.append(send(queries(1)))

    rate_all = both(rate_sent)
    kv_all = [both(kv_sent[0])]
    state_all = both(state_sent)
    full_rows = CORES * CORES * fast_weights.shape[2]
    square = (3, full_rows, width)
    tokens = CORES * CORES * rows
    learn_scratch = [pltpu.VMEM((tokens, width), jnp.bfloat16) for _ in range(5)]
    learn_flops = 12 * tokens * width * width
    weight_one, moment_one, casted = call(
        first_kernel,
        [*kv_all[0], *rate_all, *state_all],
        [
            jax.ShapeDtypeStruct(square, jnp.float32),
            jax.ShapeDtypeStruct(square, jnp.float32),
            jax.ShapeDtypeStruct(square, jnp.bfloat16),
        ],
        [pltpu.VMEM((6, full_rows, width), jnp.bfloat16), *learn_scratch],
        "learn_first",
        learn_flops,
    )

    def answer(period, casted):
        before = kv_all[max(period - 1, 0)][2:]
        return call(
            functools.partial(query_kernel, period),
            [*query_sent[period], *kv_all[period], *before, casted, fast_gain, gain_other],
            [jax.ShapeDtypeStruct((rows, width), jnp.bfloat16)] * CORES,
            [],
            f"answer_{period}",
            6 * CORES * rows * width * width,
        )

    out_sent = [send_home(answer(0, casted))]
    kv_all.append(both(kv_sent[1]))
    casted, *state_back = call(
        second_kernel,
        [*kv_all[1], *rate_all, weight_one, moment_one, casted],
        [
            jax.ShapeDtypeStruct(square, jnp.bfloat16),
            *[jax.ShapeDtypeStruct((6, fast_weights.shape[2], width), jnp.bfloat16)] * CORES,
        ],
        [pltpu.VMEM((full_rows, width), jnp.bfloat16), *learn_scratch],
        "learn_second",
        learn_flops,
    )
    state_home = send_home(state_back)
    out_sent.append(send_home(answer(1, casted)))
    state_new = jnp.stack(by_turn(*state_home), axis=1).astype(jnp.float32)
    layer_out = jnp.stack([jnp.concatenate(by_turn(*pair), axis=1) for pair in out_sent])
    return (layer_out, state_new[:3], state_new[3:])


def shifted(block, axis, distance):
    devices = range(lax.axis_size(axis))
    route = [((i - distance) % len(devices), i) for i in devices]
    return lax.ppermute(block, axis, route)


def attend(query_rows, key_rows, value_rows, halo_live, head_count):
    periods, row_count, features = query_rows.shape
    key_span = key_rows.shape[1]
    query_heads = query_rows.reshape(periods, row_count, head_count, HD)
    key_heads = key_rows.reshape(periods, key_span, head_count, HD)
    value_heads = value_rows.reshape(periods, key_span, head_count, HD)
    scores = jnp.einsum(
        "pqhd,pkhd->phqk", query_heads, key_heads, preferred_element_type=jnp.float32
    )
    scores = scores * (1.0 / math.sqrt(HD))
    query_pos = lax.broadcasted_iota(jnp.int32, (row_count, key_span), 0)
    key_pos = lax.broadcasted_iota(jnp.int32, (row_count, key_span), 1) - (key_span - row_count)
    band = (key_pos <= query_pos) & (key_pos > query_pos - WINDOW)
    allowed = band[None] & ((key_pos >= 0)[None] | halo_live[:, None, None])
    scores = jnp.where(allowed[:, None], scores, -1e30)
    top = jnp.max(scores, axis=-1, keepdims=True)
    expo = jnp.exp(scores - top)
    probs = (expo / jnp.sum(expo, axis=-1, keepdims=True)).astype(jnp.bfloat16)
    mixed = jnp.einsum("phqk,pkhd->pqhd", probs, value_heads, preferred_element_type=jnp.float32)
    return mixed.reshape(periods, row_count, features)


def silu_parts(pre):
    sigma = jax.nn.sigmoid(pre)
    return (pre * sigma, sigma * (1.0 + pre * (1.0 - sigma)))


def partial_grads(casted, key_norm, targets):
    gate_pre = jnp.einsum("thi,hji->htj", key_norm, casted[0], preferred_element_type=jnp.float32)
    up_pre = jnp.einsum("thi,hji->htj", key_norm, casted[1], preferred_element_type=jnp.float32)
    active, slope = silu_parts(gate_pre)
    hidden = (active * up_pre).astype(jnp.bfloat16)
    back = -jnp.einsum("tho,hoj->htj", targets, casted[2], preferred_element_type=jnp.float32)
    d_gate = (back * up_pre * slope).astype(jnp.bfloat16)
    d_up = (back * active).astype(jnp.bfloat16)
    g_gate = jnp.einsum("htj,thi->hji", d_gate, key_norm, preferred_element_type=jnp.float32)
    g_up = jnp.einsum("htj,thi->hji", d_up, key_norm, preferred_element_type=jnp.float32)
    g_down = -jnp.einsum("tho,htj->hoj", targets, hidden, preferred_element_type=jnp.float32)
    return jnp.stack([g_gate, g_up, g_down])


def apply_fast(casted, query_norm, fast_gain):
    gate_pre = jnp.einsum("thi,hji->htj", query_norm, casted[0], preferred_element_type=jnp.float32)
    up_pre = jnp.einsum("thi,hji->htj", query_norm, casted[1], preferred_element_type=jnp.float32)
    hidden = (jax.nn.silu(gate_pre) * up_pre).astype(jnp.bfloat16)
    result = jnp.einsum("htj,hoj->tho", hidden, casted[2], preferred_element_type=jnp.float32)
    return rms_rows(result) * fast_gain[None]


def advance(weights, moment, summed, rate_total):
    moment = MOMENT_DECAY * moment + summed / rate_total[None, :, None, None]
    weights = weights - STEP_RATE * rms_rows(moment)
    return (weights, moment)


def spread_rows(weights):
    return lax.all_gather(weights.astype(jnp.bfloat16), "seq", axis=2, tiled=True)


def row_parallel(token_queries, token_keys, token_values, step_size, fast_weights, momentum, fast_gain):
    periods, row_count, features = token_queries.shape
    head_count = features // HD
    head_width = fast_weights.shape[3]
    fast_heads = features // head_width
    seq_place = lax.axis_index("seq")
    leading = seq_place == 0
    tail_rows = shifted((token_keys, token_values), "seq", 1)
    halo_keys = jnp.where(leading, jnp.roll(tail_rows[0], 1, axis=0), tail_rows[0])
    halo_values = jnp.where(leading, jnp.roll(tail_rows[1], 1, axis=0), tail_rows[1])
    halo_live = jnp.logical_or(jnp.logical_not(leading), jnp.arange(periods, dtype=jnp.int32) > 0)
    key_all = jnp.concatenate([halo_keys, token_keys], 1)
    value_all = jnp.concatenate([halo_values, token_values], 1)
    mixed_all = attend(token_queries, key_all, value_all, halo_live, head_count)
    weight_state, moment_state = (fast_weights, momentum)
    casted = spread_rows(weight_state)
    outputs = []
    for period in range(periods):
        rates = step_size[:, period]
        key_norm = rms_rows(
            token_keys[period].reshape(row_count, fast_heads, head_width).astype(jnp.float32)
        ).astype(jnp.bfloat16)
        targets = (
            rates.T[:, :, None]
            * token_values[period].reshape(row_count, fast_heads, head_width).astype(jnp.float32)
        ).astype(jnp.bfloat16)
        partial_value = partial_grads(casted, key_norm, targets)
        rate_total = lax.psum(jnp.sum(rates, axis=1), "seq")
        summed = lax.psum_scatter(
            partial_value.astype(jnp.bfloat16), "seq", scatter_dimension=2, tiled=True
        ).astype(jnp.float32)
        weight_state, moment_state = advance(weight_state, moment_state, summed, rate_total)
        casted = spread_rows(weight_state)
        query_norm = rms_rows(
            token_queries[period].reshape(row_count, fast_heads, head_width).astype(jnp.float32)
        ).astype(jnp.bfloat16)
        fast_out = apply_fast(casted, query_norm, fast_gain).reshape(row_count, features)
        outputs.append((mixed_all[period] + fast_out).astype(jnp.bfloat16))
    return (jnp.stack(outputs), weight_state, moment_state)


def shards(token_queries, token_keys, token_values, step_size, fast_weights, momentum, fast_gain):
    _, rows, features = token_queries.shape
    heads = features // fast_weights.shape[3]
    fits = heads == CORES and lax.axis_size("seq") == heads * CORES and lax.axis_size("head") % CORES == 0
    plan = head_parallel if fits and rows == WINDOW else row_parallel
    return plan(token_queries, token_keys, token_values, step_size, fast_weights, momentum, fast_gain)


def solution(mesh):
    placed = (
        P("grp", "seq", "head"),
        P("grp", "seq", "head"),
        P("grp", "seq", "head"),
        P("head", "grp", "seq"),
        P("grp", "head", "seq", None),
        P("grp", "head", "seq", None),
        P("head", None),
    )
    return jax.shard_map(
        shards,
        mesh=mesh,
        in_specs=placed,
        out_specs=(
            P("grp", "seq", "head"),
            P("grp", "head", "seq", None),
            P("grp", "head", "seq", None),
        ),
        check_vma=False,
    )
```
